32 devices in a mesh: dp: 8 (over z, y), expert: 2 (over core), tensor: 2 (over x).
Axes of the slice: x: 2, y: 2, z: 4, core: 2. Of those that a mesh axis runs over, the one named last changes fastest.
Arguments:
- dense_act: bfloat16 [2, 32, 512, 3584], P(None, 'dp', 'expert', 'tensor'), may hold values from -6 to 6
- dense_cot: bfloat16 [2, 32, 512, 3584], P(None, 'dp', ('expert', 'tensor')), may hold values from -6 to 6
- dense_proj_in: bfloat16 [2, 3584, 128], P(None, 'tensor'), may hold values from -0.09375 to 0.09375
- dense_proj_out: bfloat16 [2, 3584, 128], replicated, may hold values from -0.09375 to 0.09375
- expert_act: bfloat16 [32, 8, 64, 2560], P('dp', 'expert', None, 'tensor'), may hold values from -6 to 6
- expert_cot: bfloat16 [32, 8, 64, 3584], P('dp', 'expert', 'tensor'), may hold values from -6 to 6
- expert_proj_in: bfloat16 [2560, 128], P('tensor'), may hold values from -0.125 to 0.125
- expert_proj_out: bfloat16 [3584, 128], replicated, may hold values from -0.09375 to 0.09375
- dense_valid: float32 [2, 128, 128], replicated, may hold values from -0.0012207031 to 0.0012207031
- expert_valid: float32 [8, 128, 128], P('expert'), may hold values from -0.0012207031 to 0.0012207031
- domain_ids: int32 [32], P('dp'), may hold values from 0 to 63
- prior_mix: float32 [64], replicated, may hold values from 0.002 to 0.05
Outputs:
- log_mixture_weights: float32 [64], P('dp')
The draws below stay inside these ranges and needn't reach their ends.
All inputs are finite; a program needn't handle non-finite values.
Results may differ from the reference program's by a relative error of at most 0.0003.
Values sent between devices are 32-bit elements; how exact they have to be, the bound alone decides.
No kernel may reach another device: no remote copies, remote signals or barrier semaphores. Data moves between devices by JAX's collectives and lax.ppermute only.
A program may use at most 128 MiB of HBM per device.

```python
import math
import jax
import jax.numpy as jnp
from jax import lax

D = 3584
FFE = 2560
R = 128
LAYERS = 2
DOMAINS = 64
TOK_MB = 512
CAP = 64
MICRO = 32
EXPERTS = 8


def plant(array, own_key, low, high):
    place = [jax.random.randint(jax.random.fold_in(own_key, axis), (), 0, length) for axis, length in enumerate(array.shape)]
    main_axis = array.shape.index(max(array.shape))
    neighbour = place[:main_axis] + [(place[main_axis] + 1) % array.shape[main_axis]] + place[main_axis + 1:]
    return array.at[tuple(place)].set(low).at[tuple(neighbour)].set(high)


def steps_of(own_key, extent, cuts, smallest, high):
    def one(position, shards_of):
        heights = jax.random.uniform(jax.random.fold_in(jax.random.fold_in(own_key, 6), position), (shards_of,), jnp.float32, smallest / len(cuts), high / len(cuts))
        return jnp.repeat(jnp.exp(heights), extent[position] // shards_of).reshape((-1,) + (1,) * (len(extent) - position - 1))

    loudness = one(*cuts[0])
    for cut in cuts[1:]:
        loudness = loudness * one(*cut)
    return loudness


def gaussian(key, shape, scale, reach, split=(), kind=jnp.bfloat16):
    entries = jax.random.normal(key, shape, jnp.float32) * scale
    if len(split) > 0:
        entries = steps_of(key, shape, split, -0.22, 0.18) * entries
    return jnp.clip(entries, min=-reach, max=reach).astype(kind)


def setup_inputs(seed: int = 0) -> dict:
    key_list = jax.random.split(jax.random.key(seed), 13)
    dense_act = gaussian(key_list[0], (LAYERS, MICRO, TOK_MB, D), 1.0, 6.0, ((1, 8), (2, 2), (3, 2)))
    dense_cot = gaussian(key_list[1], (LAYERS, MICRO, TOK_MB, D), 1.0, 6.0, ((1, 8), (2, 4)))
    dense_proj_in = gaussian(key_list[2], (LAYERS, D, R), D ** -0.5, 0.09375, ((1, 2),))
    dense_proj_out = gaussian(key_list[3], (LAYERS, D, R), D ** -0.5, 0.09375)
    expert_act = gaussian(key_list[4], (MICRO, EXPERTS, CAP, FFE), 1.0, 6.0, ((0, 8), (1, 2), (3, 2)))
    expert_cot = gaussian(key_list[5], (MICRO, EXPERTS, CAP, D), 1.0, 6.0, ((0, 8), (1, 2), (2, 2)))
    expert_proj_in = gaussian(key_list[6], (FFE, R), FFE ** -0.5, 0.125, ((0, 2),))
    expert_proj_out = gaussian(key_list[7], (D, R), D ** -0.5, 0.09375)
    dense_valid = gaussian(key_list[8], (LAYERS, R, R), (R * R * (LAYERS * TOK_MB + EXPERTS * CAP)) ** -0.5, 0.0012207031, (), jnp.float32)
    expert_valid = gaussian(key_list[9], (EXPERTS, R, R), (R * R * (LAYERS * TOK_MB + EXPERTS * CAP)) ** -0.5, 0.0012207031, ((0, 2),), jnp.float32)
    domain_ids = plant(jax.random.randint(key_list[10], (MICRO,), 0, DOMAINS), jax.random.fold_in(key_list[10], 1), 0, DOMAINS - 1).astype(jnp.int32)
    prior_mix = jnp.clip(jnp.exp(jax.random.uniform(key_list[11], (DOMAINS,), jnp.float32, math.log(0.002), math.log(0.05))), 0.002, 0.05)
    return dict(dense_act=dense_act, dense_cot=dense_cot, dense_proj_in=dense_proj_in, dense_proj_out=dense_proj_out, expert_act=expert_act, expert_cot=expert_cot, expert_proj_in=expert_proj_in, expert_proj_out=expert_proj_out, dense_valid=dense_valid, expert_valid=expert_valid, domain_ids=domain_ids, prior_mix=prior_mix)


def reference(dense_act, dense_cot, dense_proj_in, dense_proj_out, expert_act, expert_cot, expert_proj_in, expert_proj_out, dense_valid, expert_valid, domain_ids, prior_mix):
    width = dense_act.shape[3]
    micro = dense_act.shape[1]
    tokens = dense_act.shape[2]
    rank = dense_proj_in.shape[2]
    score = jnp.zeros((micro,), jnp.float32)
    for layer in range(dense_act.shape[0]):
        dense_update_vector = jnp.dot(dense_act[layer].reshape(-1, width), dense_proj_in[layer], preferred_element_type=jnp.float32).reshape(micro, tokens, rank)
        dense_weight_matrix = jnp.dot(dense_cot[layer].reshape(-1, width), dense_proj_out[layer], preferred_element_type=jnp.float32).reshape(micro, tokens, rank)
        sketch = jnp.einsum('mtr,mts->mrs', dense_update_vector, dense_weight_matrix, precision=lax.Precision.HIGHEST)
        score = score + lax.optimization_barrier(jnp.sum(sketch * dense_valid[layer][None], axis=(1, 2)))
    experts = expert_act.shape[1]
    slots = expert_act.shape[2]
    expert_u = jnp.dot(expert_act.reshape(-1, expert_act.shape[3]), expert_proj_in, preferred_element_type=jnp.float32).reshape(micro, experts, slots, rank)
    expert_weight_matrix = jnp.dot(expert_cot.reshape(-1, width), expert_proj_out, preferred_element_type=jnp.float32).reshape(micro, experts, slots, rank)
    expert_sketch = jnp.einsum('mecr,mecs->mers', expert_u, expert_weight_matrix, precision=lax.Precision.HIGHEST)
    score = score + lax.optimization_barrier(jnp.sum(expert_sketch * expert_valid[None], axis=(1, 2, 3)))
    domains = prior_mix.shape[0]
    onehot = (domain_ids[:, None] == jnp.arange(domains, dtype=jnp.int32)[None, :]).astype(jnp.float32)
    domain_total = jnp.dot(score, onehot, precision=lax.Precision.HIGHEST)
    spread = jnp.sqrt(jnp.mean(domain_total * domain_total) + 1e-06)
    z_value = domain_total / spread
    mass = jnp.sum(prior_mix * jnp.exp(0.5 * z_value))
    return jnp.log(prior_mix) + 0.5 * z_value - jnp.log(mass)
```

```python
import functools

import jax
import jax.numpy as jnp
from jax import lax
from jax.experimental import pallas as pl
from jax.experimental.pallas import tpu as pltpu
from jax.sharding import PartitionSpec as P


AXES = ("dp", "expert", "tensor")
HBM = pl.BlockSpec(memory_space=pltpu.HBM)
ANY = pl.BlockSpec(memory_space=pl.ANY)
VMEM = pl.BlockSpec(memory_space=pltpu.VMEM)
SMEM = pl.BlockSpec(memory_space=pltpu.SMEM)


def vmem(mib):
    return pltpu.CompilerParams(vmem_limit_bytes=mib * 2**20)


def start_all(pairs, sems):
    copies = [pltpu.make_async_copy(src, dst, sems.at[i]) for i, (src, dst) in enumerate(pairs)]
    for copy in copies:
        copy.start()
    return copies


def dot(a, b):
    return jnp.dot(a, b, preferred_element_type=jnp.float32)


def dot_exact(a, b):
    return lax.dot_general(
        a, b, (((1,), (1,)), ((), ())), precision=lax.Precision.HIGHEST, preferred_element_type=jnp.float32
    )


def expert_send_kernel(act, proj, out, act_v, proj_v, sems):
    micro, experts, rows, width = act_v.shape
    first = (1 - lax.axis_index("tensor")) * rows
    copies = start_all(
        [(proj, proj_v)] + [(act.at[m, :, pl.ds(first, rows), :], act_v.at[m]) for m in range(micro)], sems
    )
    copies[0].wait()
    for m in range(micro):
        copies[1 + m].wait()
        u = dot(act_v[m].reshape(experts * rows, width), proj_v[...])
        out[m] = u.reshape(experts, rows, -1)


def dense_send_kernel(act, proj, _after, out, act_v, proj_v, sems):
    layers, micro, rows, _ = act_v.shape
    first = (1 - lax.axis_index("tensor")) * rows
    pairs = []
    for l in range(layers):
        pairs.append((proj.at[l], proj_v.at[l]))
        pairs += [(act.at[l, m, pl.ds(first, rows), :], act_v.at[l, m]) for m in range(micro)]
    copies = start_all(pairs, sems)
    for l in range(layers):
        copies[l * (micro + 1)].wait()
        for m in range(micro):
            copies[l * (micro + 1) + 1 + m].wait()
            out[l, m] = dot(act_v[l, m], proj_v[l])


def own_kernel(
    dact, dcot, dpin, dpout, eact, ecot, epin, epout, dval, evaldn,
    yd, ye, own,
    dact_v, dcot_v, dpin_v, dpout_v, eact_v, ecot_v, epin_v, epout_v, dval_v, eval_v, sems,
):
    layers, micro, rows, _ = dact_v.shape
    _, experts, slots, ewidth = eact_v.shape
    rank = dval_v.shape[-1]
    tensor = lax.axis_index("tensor")
    pairs = []
    for l in range(layers):
        pairs += [(dpout.at[l], dpout_v.at[l]), (dval.at[l], dval_v.at[l]), (dpin.at[l], dpin_v.at[l])]
        for m in range(micro):
            pairs += [
                (dcot.at[l, m], dcot_v.at[l, m]),
                (dact.at[l, m, pl.ds(tensor * rows, rows), :], dact_v.at[l, m]),
            ]
    pairs += [(epout, epout_v), (evaldn, eval_v), (epin, epin_v)]
    for m in range(micro):
        pairs += [
            (ecot.at[m], ecot_v.at[m]),
            (eact.at[m, :, pl.ds(tensor * slots, slots), :], eact_v.at[m]),
        ]
    copies = iter(start_all(pairs, sems))
    totals = [jnp.zeros((1, rank), jnp.float32) for _ in range(micro)]
    for l in range(layers):
        for _ in range(3):
            next(copies).wait()
        for m in range(micro):
            next(copies).wait()
            w = dot(dcot_v[l, m], dpout_v[l])
            y = dot_exact(w, dval_v[l])
            yd[l, m] = y
            next(copies).wait()
            u = dot(dact_v[l, m], dpin_v[l])
            totals[m] = totals[m] + jnp.sum(u * y, axis=0, keepdims=True)
    for _ in range(3):
        next(copies).wait()
    for m in range(micro):
        next(copies).wait()
        w = dot(ecot_v[m].reshape(experts * slots, -1), epout_v[...])
        next(copies).wait()
        u = dot(eact_v[m].reshape(experts * slots, ewidth), epin_v[...])
        for e in range(experts):
            part = slice(e * slots, (e + 1) * slots)
            y = dot_exact(w[part], eval_v[e])
            ye[m, e] = y
            totals[m] = totals[m] + jnp.sum(u[part] * y, axis=0, keepdims=True)
    own[...] = jnp.concatenate(totals, axis=0)


def combine_kernel(ids, own, ud, yd, ue, ye, out):
    layers, micro = ud.shape[:2]
    domains = out.shape[-1]
    lane = lax.broadcasted_iota(jnp.int32, (1, domains), 1)
    total = jnp.zeros((1, domains), jnp.float32)
    for m in range(micro):
        part = own[pl.ds(m, 1), :]
        for l in range(layers):
            part = part + jnp.sum(ud[l, m] * yd[l, m], axis=0, keepdims=True)
        experts, slots, rank = ue.shape[1:]
        e_prod = ue[m].reshape(experts * slots, rank) * ye[m].reshape(experts * slots, rank)
        part = part + jnp.sum(e_prod, axis=0, keepdims=True)
        score = jnp.sum(part, axis=1, keepdims=True)
        total = total + jnp.where(lane == ids[m], score, 0.0)
    out[...] = jnp.broadcast_to(total, out.shape)


def final_kernel(parts, prior, out, wide):
    domains = prior.shape[-1]
    share = out.shape[-1]
    total = jnp.sum(parts[...], axis=0, keepdims=True)
    spread = jnp.sqrt(jnp.mean(total * total, axis=1, keepdims=True) + 1e-06)
    half = 0.5 * (total / spread)
    mass = jnp.sum(prior[...] * jnp.exp(half), axis=1, keepdims=True)
    lanes = wide.shape[-1]
    wide[...] = jnp.zeros_like(wide)
    wide[:, :domains] = jnp.log(prior[...]) + half - jnp.log(mass)
    first = lax.axis_index("dp") * share
    out[...] = pltpu.roll(wide[...], lax.rem(lanes - first, lanes), 1)[:, :share]


def per_device(
    dense_act,
    dense_cot,
    dense_proj_in,
    dense_proj_out,
    expert_act,
    expert_cot,
    expert_proj_in,
    expert_proj_out,
    dense_valid,
    expert_valid,
    domain_ids,
    prior_mix,
):
    layers, micro, rows, dwidth = dense_cot.shape
    experts, slots = expert_cot.shape[1:3]
    d_in = dense_act.shape[3]
    e_in = expert_act.shape[3]
    rank = dense_proj_in.shape[2]
    domains = prior_mix.shape[0]
    world = lax.axis_size(AXES)
    n_tensor = lax.axis_size("tensor")
    swap = [(i, i ^ 1) for i in range(n_tensor)]
    f32, bf16 = jnp.float32, jnp.bfloat16
    dma = pltpu.SemaphoreType.DMA

    hbm = functools.partial(pltpu.with_memory_space_constraint, memory_space=pltpu.HBM)
    dense_act, dense_cot, dense_proj_in, dense_proj_out = map(
        hbm, (dense_act, dense_cot, dense_proj_in, dense_proj_out)
    )
    expert_act, expert_cot, expert_proj_in, expert_proj_out = map(
        hbm, (expert_act, expert_cot, expert_proj_in, expert_proj_out)
    )
    dense_valid, expert_valid = hbm(dense_valid), hbm(expert_valid)

    e_send = pl.pallas_call(
        expert_send_kernel,
        out_shape=jax.ShapeDtypeStruct((micro, experts, slots, rank), f32),
        in_specs=[HBM, HBM],
        out_specs=VMEM,
        scratch_shapes=[
            pltpu.VMEM((micro, experts, slots, e_in), bf16),
            pltpu.VMEM((e_in, rank), bf16),
            dma((micro + 1,)),
        ],
        compiler_params=vmem(4),
        name="expert_send",
    )(expert_act, expert_proj_in)
    e_got = lax.ppermute(e_send, "tensor", swap)

    d_send = pl.pallas_call(
        dense_send_kernel,
        out_shape=jax.ShapeDtypeStruct((layers, micro, rows, rank), f32),
        in_specs=[HBM, HBM, ANY],
        out_specs=VMEM,
        scratch_shapes=[
            pltpu.VMEM((layers, micro, rows, d_in), bf16),
            pltpu.VMEM((layers, d_in, rank), bf16),
            dma((layers * (micro + 1),)),
        ],
        compiler_params=vmem(8),
        name="dense_send",
    )(dense_act, dense_proj_in, e_send)
    d_got = lax.ppermute(d_send, "tensor", swap)

    y_d, y_e, own = pl.pallas_call(
        own_kernel,
        out_shape=[
            jax.ShapeDtypeStruct((layers, micro, rows, rank), f32),
            jax.ShapeDtypeStruct((micro, experts, slots, rank), f32),
            jax.ShapeDtypeStruct((micro, rank), f32),
        ],
        in_specs=[HBM] * 10,
        out_specs=[VMEM] * 3,
        scratch_shapes=[
            pltpu.VMEM((layers, micro, rows, d_in), bf16),
            pltpu.VMEM((layers, micro, rows, dwidth), bf16),
            pltpu.VMEM((layers, d_in, rank), bf16),
            pltpu.VMEM((layers, dwidth, rank), bf16),
            pltpu.VMEM((micro, experts, slots, e_in), bf16),
            pltpu.VMEM((micro, experts, slots, dwidth), bf16),
            pltpu.VMEM((e_in, rank), bf16),
            pltpu.VMEM((dwidth, rank), bf16),
            pltpu.VMEM((layers, rank, rank), f32),
            pltpu.VMEM((experts, rank, rank), f32),
            dma((layers * (3 + 2 * micro) + 3 + 2 * micro,)),
        ],
        compiler_params=vmem(32),
        name="own_part",
    )(
        dense_act, dense_cot, dense_proj_in, dense_proj_out,
        expert_act, expert_cot, expert_proj_in, expert_proj_out, dense_valid, expert_valid,
    )

    parts = pl.pallas_call(
        combine_kernel,
        out_shape=jax.ShapeDtypeStruct((world, domains), f32),
        in_specs=[SMEM] + [VMEM] * 5,
        out_specs=VMEM,
        compiler_params=vmem(6),
        name="combine",
    )(domain_ids, own, d_got, y_d, e_got, y_e)
    parts = lax.all_to_all(parts, AXES, 0, 0, tiled=True)

    share = domains // lax.axis_size("dp")
    lanes = -(-domains // 128) * 128
    out = pl.pallas_call(
        final_kernel,
        out_shape=jax.ShapeDtypeStruct((1, share), f32),
        in_specs=[VMEM, VMEM],
        out_specs=VMEM,
        scratch_shapes=[pltpu.VMEM((1, lanes), f32)],
        compiler_params=vmem(1),
        name="final",
    )(parts, prior_mix.reshape(1, domains))
    return out.reshape(share)


def solution(mesh):
    placed = (
        P(None, "dp", "expert", "tensor"),
        P(None, "dp", ("expert", "tensor"), None),
        P(None, "tensor", None),
        P(),
        P("dp", "expert", None, "tensor"),
        P("dp", "expert", "tensor", None),
        P("tensor", None),
        P(),
        P(),
        P("expert", None, None),
        P("dp"),
        P(),
    )

    return jax.shard_map(per_device, mesh=mesh, in_specs=placed, out_specs=P("dp"), check_vma=False)
```

```python
import functools

import jax
import jax.numpy as jnp
from jax import lax
from jax.experimental import pallas as pl
from jax.experimental.pallas import tpu as pltpu
from jax.sharding import PartitionSpec as P


AXES = ("dp", "expert", "tensor")
HBM = pl.BlockSpec(memory_space=pltpu.HBM)
ANY = pl.BlockSpec(memory_space=pl.ANY)
VMEM = pl.BlockSpec(memory_space=pltpu.VMEM)
SMEM = pl.BlockSpec(memory_space=pltpu.SMEM)


def vmem(mib):
    return pltpu.CompilerParams(vmem_limit_bytes=mib * 2**20)


def start_all(pairs, sems):
    copies = [pltpu.make_async_copy(src, dst, sems.at[i]) for i, (src, dst) in enumerate(pairs)]
    for copy in copies:
        copy.start()
    return copies


def dot(a, b):
    return jnp.dot(a, b, preferred_element_type=jnp.float32)


def dot_exact(a, b):
    return lax.dot_general(
        a, b, (((1,), (1,)), ((), ())), precision=lax.Precision.HIGHEST, preferred_element_type=jnp.float32
    )


def expert_send_kernel(act, proj, out, act_v, proj_v, sems):
    micro, experts, rows, width = act_v.shape
    first = (1 - lax.axis_index("tensor")) * rows
    copies = start_all(
        [(proj, proj_v)] + [(act.at[m, :, pl.ds(first, rows), :], act_v.at[m]) for m in range(micro)], sems
    )
    for copy in copies:
        copy.wait()
    u = dot(act_v[...].reshape(micro * experts * rows, width), proj_v[...])
    out[...] = u.reshape(out.shape)


def dense_send_kernel(act, proj, _after, out, act_v, proj_v, sems):
    layers, micro, rows, width = act_v.shape
    first = (1 - lax.axis_index("tensor")) * rows
    pairs = []
    for l in range(layers):
        pairs.append((proj.at[l], proj_v.at[l]))
        pairs += [(act.at[l, m, pl.ds(first, rows), :], act_v.at[l, m]) for m in range(micro)]
    copies = iter(start_all(pairs, sems))
    for l in range(layers):
        for _ in range(1 + micro):
            next(copies).wait()
        out[l] = dot(act_v[l].reshape(micro * rows, width), proj_v[l]).reshape(micro, rows, -1)


def own_kernel(
    dact, dcot, dpin, dpout, eact, ecot, epin, epout, dval, evaldn,
    yd, ye, own,
    dact_v, dcot_v, dpin_v, dpout_v, eact_v, ecot_v, epin_v, epout_v, dval_v, eval_v, sems,
):
    layers, micro, rows, dwidth = dact_v.shape
    _, experts, slots, ewidth = eact_v.shape
    rank = dval_v.shape[-1]
    tensor = lax.axis_index("tensor")
    pairs = [(epout, epout_v), (evaldn, eval_v), (epin, epin_v)]
    for m in range(micro):
        pairs += [
            (ecot.at[m], ecot_v.at[m]),
            (eact.at[m, :, pl.ds(tensor * slots, slots), :], eact_v.at[m]),
        ]
    for l in range(layers):
        pairs += [(dpout.at[l], dpout_v.at[l]), (dval.at[l], dval_v.at[l]), (dpin.at[l], dpin_v.at[l])]
        for m in range(micro):
            pairs += [
                (dcot.at[l, m], dcot_v.at[l, m]),
                (dact.at[l, m, pl.ds(tensor * rows, rows), :], dact_v.at[l, m]),
            ]
    copies = iter(start_all(pairs, sems))
    totals = [jnp.zeros((1, rank), jnp.float32) for _ in range(micro)]
    for _ in range(3 + 2 * micro):
        next(copies).wait()
    w = dot(ecot_v[...].reshape(micro * experts * slots, -1), epout_v[...])
    u = dot(eact_v[...].reshape(micro * experts * slots, ewidth), epin_v[...])
    for e in range(experts):
        places = [slice((m * experts + e) * slots, (m * experts + e + 1) * slots) for m in range(micro)]
        y = dot_exact(jnp.concatenate([w[place] for place in places], axis=0), eval_v[e])
        for m in range(micro):
            y_m = y[m * slots : (m + 1) * slots]
            ye[m, e] = y_m
            totals[m] = totals[m] + jnp.sum(u[places[m]] * y_m, axis=0, keepdims=True)
    for l in range(layers):
        for _ in range(3 + 2 * micro):
            next(copies).wait()
        w = dot(dcot_v[l].reshape(micro * rows, -1), dpout_v[l])
        u = dot(dact_v[l].reshape(micro * rows, dwidth), dpin_v[l])
        y = dot_exact(w, dval_v[l])
        for m in range(micro):
            place = slice(m * rows, (m + 1) * rows)
            yd[l, m] = y[place]
            totals[m] = totals[m] + jnp.sum(u[place] * y[place], axis=0, keepdims=True)
    own[...] = jnp.concatenate(totals, axis=0)


def combine_kernel(ids, own, ud, yd, ue, ye, out):
    layers, micro = ud.shape[:2]
    domains = out.shape[-1]
    lane = lax.broadcasted_iota(jnp.int32, (1, domains), 1)
    total = jnp.zeros((1, domains), jnp.float32)
    for m in range(micro):
        part = own[pl.ds(m, 1), :]
        for l in range(layers):
            part = part + jnp.sum(ud[l, m] * yd[l, m], axis=0, keepdims=True)
        experts, slots, rank = ue.shape[1:]
        e_prod = ue[m].reshape(experts * slots, rank) * ye[m].reshape(experts * slots, rank)
        part = part + jnp.sum(e_prod, axis=0, keepdims=True)
        score = jnp.sum(part, axis=1, keepdims=True)
        total = total + jnp.where(lane == ids[m], score, 0.0)
    out[...] = jnp.broadcast_to(total, out.shape)


def final_kernel(parts, prior, out, wide):
    domains = prior.shape[-1]
    share = out.shape[-1]
    total = jnp.sum(parts[...], axis=0, keepdims=True)
    spread = jnp.sqrt(jnp.mean(total * total, axis=1, keepdims=True) + 1e-06)
    half = 0.5 * (total / spread)
    mass = jnp.sum(prior[...] * jnp.exp(half), axis=1, keepdims=True)
    lanes = wide.shape[-1]
    wide[...] = jnp.zeros_like(wide)
    wide[:, :domains] = jnp.log(prior[...]) + half - jnp.log(mass)
    first = lax.axis_index("dp") * share
    out[...] = pltpu.roll(wide[...], lax.rem(lanes - first, lanes), 1)[:, :share]


def per_device(
    dense_act,
    dense_cot,
    dense_proj_in,
    dense_proj_out,
    expert_act,
    expert_cot,
    expert_proj_in,
    expert_proj_out,
    dense_valid,
    expert_valid,
    domain_ids,
    prior_mix,
):
    layers, micro, rows, dwidth = dense_cot.shape
    experts, slots = expert_cot.shape[1:3]
    d_in = dense_act.shape[3]
    e_in = expert_act.shape[3]
    rank = dense_proj_in.shape[2]
    domains = prior_mix.shape[0]
    world = lax.axis_size(AXES)
    n_tensor = lax.axis_size("tensor")
    swap = [(i, i ^ 1) for i in range(n_tensor)]
    f32, bf16 = jnp.float32, jnp.bfloat16
    dma = pltpu.SemaphoreType.DMA

    hbm = functools.partial(pltpu.with_memory_space_constraint, memory_space=pltpu.HBM)
    dense_act, dense_cot, dense_proj_in, dense_proj_out = map(
        hbm, (dense_act, dense_cot, dense_proj_in, dense_proj_out)
    )
    expert_act, expert_cot, expert_proj_in, expert_proj_out = map(
        hbm, (expert_act, expert_cot, expert_proj_in, expert_proj_out)
    )
    dense_valid, expert_valid = hbm(dense_valid), hbm(expert_valid)

    e_send = pl.pallas_call(
        expert_send_kernel,
        out_shape=jax.ShapeDtypeStruct((micro, experts, slots, rank), f32),
        in_specs=[HBM, HBM],
        out_specs=VMEM,
        scratch_shapes=[
            pltpu.VMEM((micro, experts, slots, e_in), bf16),
            pltpu.VMEM((e_in, rank), bf16),
            dma((micro + 1,)),
        ],
        compiler_params=vmem(4),
        name="expert_send",
    )(expert_act, expert_proj_in)
    e_got = lax.ppermute(e_send, "tensor", swap)

    d_send = pl.pallas_call(
        dense_send_kernel,
        out_shape=jax.ShapeDtypeStruct((layers, micro, rows, rank), f32),
        in_specs=[HBM, HBM, ANY],
        out_specs=VMEM,
        scratch_shapes=[
            pltpu.VMEM((layers, micro, rows, d_in), bf16),
            pltpu.VMEM((layers, d_in, rank), bf16),
            dma((layers * (micro + 1),)),
        ],
        compiler_params=vmem(8),
        name="dense_send",
    )(dense_act, dense_proj_in, e_send)
    d_got = lax.ppermute(d_send, "tensor", swap)

    y_d, y_e, own = pl.pallas_call(
        own_kernel,
        out_shape=[
            jax.ShapeDtypeStruct((layers, micro, rows, rank), f32),
            jax.ShapeDtypeStruct((micro, experts, slots, rank), f32),
            jax.ShapeDtypeStruct((micro, rank), f32),
        ],
        in_specs=[HBM] * 10,
        out_specs=[VMEM] * 3,
        scratch_shapes=[
            pltpu.VMEM((layers, micro, rows, d_in), bf16),
            pltpu.VMEM((layers, micro, rows, dwidth), bf16),
            pltpu.VMEM((layers, d_in, rank), bf16),
            pltpu.VMEM((layers, dwidth, rank), bf16),
            pltpu.VMEM((micro, experts, slots, e_in), bf16),
            pltpu.VMEM((micro, experts, slots, dwidth), bf16),
            pltpu.VMEM((e_in, rank), bf16),
            pltpu.VMEM((dwidth, rank), bf16),
            pltpu.VMEM((layers, rank, rank), f32),
            pltpu.VMEM((experts, rank, rank), f32),
            dma((layers * (3 + 2 * micro) + 3 + 2 * micro,)),
        ],
        compiler_params=vmem(32),
        name="own_part",
    )(
        dense_act, dense_cot, dense_proj_in, dense_proj_out,
        expert_act, expert_cot, expert_proj_in, expert_proj_out, dense_valid, expert_valid,
    )

    parts = pl.pallas_call(
        combine_kernel,
        out_shape=jax.ShapeDtypeStruct((world, domains), f32),
        in_specs=[SMEM] + [VMEM] * 5,
        out_specs=VMEM,
        compiler_params=vmem(6),
        name="combine",
    )(domain_ids, own, d_got, y_d, e_got, y_e)
    parts = lax.all_to_all(parts, AXES, 0, 0, tiled=True)

    share = domains // lax.axis_size("dp")
    lanes = -(-domains // 128) * 128
    out = pl.pallas_call(
        final_kernel,
        out_shape=jax.ShapeDtypeStruct((1, share), f32),
        in_specs=[VMEM, VMEM],
        out_specs=VMEM,
        scratch_shapes=[pltpu.VMEM((1, lanes), f32)],
        compiler_params=vmem(1),
        name="final",
    )(parts, prior_mix.reshape(1, domains))
    return out.reshape(share)


def solution(mesh):
    placed = (
        P(None, "dp", "expert", "tensor"),
        P(None, "dp", ("expert", "tensor"), None),
        P(None, "tensor", None),
        P(),
        P("dp", "expert", None, "tensor"),
        P("dp", "expert", "tensor", None),
        P("tensor", None),
        P(),
        P(),
        P("expert", None, None),
        P("dp"),
        P(),
    )

    return jax.shard_map(per_device, mesh=mesh, in_specs=placed, out_specs=P("dp"), check_vma=False)
```

```python
import functools

import jax
import jax.numpy as jnp
from jax import lax
from jax.experimental import pallas as pl
from jax.experimental.pallas import tpu as pltpu
from jax.sharding import PartitionSpec as P


AXES = ("dp", "expert", "tensor")
HBM = pl.BlockSpec(memory_space=pltpu.HBM)
ANY = pl.BlockSpec(memory_space=pl.ANY)
VMEM = pl.BlockSpec(memory_space=pltpu.VMEM)
SMEM = pl.BlockSpec(memory_space=pltpu.SMEM)


def vmem(mib):
    return pltpu.CompilerParams(vmem_limit_bytes=mib * 2**20)


def start_all(pairs, sems):
    copies = [pltpu.make_async_copy(src, dst, sems.at[i]) for i, (src, dst) in enumerate(pairs)]
    for copy in copies:
        copy.start()
    return copies


def dot(a, b):
    return jnp.dot(a, b, preferred_element_type=jnp.float32)


def dot_exact(a, b):
    return lax.dot_general(
        a, b, (((1,), (1,)), ((), ())), precision=lax.Precision.HIGHEST, preferred_element_type=jnp.float32
    )


def expert_send_kernel(act, proj, out, act_v, proj_v, sems):
    micro, experts, rows, width = act_v.shape
    first = (1 - lax.axis_index("tensor")) * rows
    copies = start_all(
        [(proj, proj_v)] + [(act.at[m, :, pl.ds(first, rows), :], act_v.at[m]) for m in range(micro)], sems
    )
    for copy in copies:
        copy.wait()
    u = dot(act_v[...].reshape(micro * experts * rows, width), proj_v[...])
    out[...] = u.reshape(out.shape)


def dense_send_kernel(act, proj, _after, out, act_v, proj_v, sems):
    layers, micro, rows, width = act_v.shape
    first = (1 - lax.axis_index("tensor")) * rows
    pairs = []
    for l in range(layers):
        pairs.append((proj.at[l], proj_v.at[l]))
        pairs += [(act.at[l, m, pl.ds(first, rows), :], act_v.at[l, m]) for m in range(micro)]
    copies = iter(start_all(pairs, sems))
    for l in range(layers):
        for _ in range(1 + micro):
            next(copies).wait()
        out[l] = dot(act_v[l].reshape(micro * rows, width), proj_v[l]).reshape(micro, rows, -1)


def own_kernel(
    ids, dact, dcot, dpin, dpout, eact, ecot, epin, epout, dval, evaldn,
    yd, ye, own, hot,
    dact_v, dcot_v, dpin_v, dpout_v, eact_v, ecot_v, epin_v, epout_v, dval_v, eval_v, sems,
):
    layers, micro, rows, dwidth = dact_v.shape
    _, experts, slots, ewidth = eact_v.shape
    rank = dval_v.shape[-1]
    tensor = lax.axis_index("tensor")
    pairs = [(epout, epout_v), (evaldn, eval_v), (epin, epin_v)]
    for m in range(micro):
        pairs += [
            (ecot.at[m], ecot_v.at[m]),
            (eact.at[m, :, pl.ds(tensor * slots, slots), :], eact_v.at[m]),
        ]
    for l in range(layers):
        pairs += [(dpout.at[l], dpout_v.at[l]), (dval.at[l], dval_v.at[l]), (dpin.at[l], dpin_v.at[l])]
        for m in range(micro):
            pairs += [
                (dcot.at[l, m], dcot_v.at[l, m]),
                (dact.at[l, m, pl.ds(tensor * rows, rows), :], dact_v.at[l, m]),
            ]
    copies = iter(start_all(pairs, sems))
    totals = [jnp.zeros((1, rank), jnp.float32) for _ in range(micro)]
    for _ in range(3 + 2 * micro):
        next(copies).wait()
    w = dot(ecot_v[...].reshape(micro * experts * slots, -1), epout_v[...])
    u = dot(eact_v[...].reshape(micro * experts * slots, ewidth), epin_v[...])
    for e in range(experts):
        places = [slice((m * experts + e) * slots, (m * experts + e + 1) * slots) for m in range(micro)]
        y = dot_exact(jnp.concatenate([w[place] for place in places], axis=0), eval_v[e])
        for m in range(micro):
            y_m = y[m * slots : (m + 1) * slots]
            ye[m, e] = y_m
            totals[m] = totals[m] + jnp.sum(u[places[m]] * y_m, axis=0, keepdims=True)
    for l in range(layers):
        for _ in range(3 + 2 * micro):
            next(copies).wait()
        w = dot(dcot_v[l].reshape(micro * rows, -1), dpout_v[l])
        u = dot(dact_v[l].reshape(micro * rows, dwidth), dpin_v[l])
        y = dot_exact(w, dval_v[l])
        for m in range(micro):
            place = slice(m * rows, (m + 1) * rows)
            yd[l, m] = y[place]
            totals[m] = totals[m] + jnp.sum(u[place] * y[place], axis=0, keepdims=True)
    own[...] = jnp.concatenate(totals, axis=0)
    lane = lax.broadcasted_iota(jnp.int32, (1, hot.shape[1]), 1)
    for m in range(micro):
        hot[pl.ds(m, 1), :] = (lane == ids[m]).astype(jnp.float32)


def combine_kernel(own, hot, ud, yd, ue, ye, out):
    layers, micro = ud.shape[:2]
    parts = []
    for m in range(micro):
        part = own[pl.ds(m, 1), :]
        for l in range(layers):
            part = part + jnp.sum(ud[l, m] * yd[l, m], axis=0, keepdims=True)
        experts, slots, rank = ue.shape[1:]
        e_prod = ue[m].reshape(experts * slots, rank) * ye[m].reshape(experts * slots, rank)
        parts.append(part + jnp.sum(e_prod, axis=0, keepdims=True))
    scores = jnp.sum(jnp.concatenate(parts, axis=0), axis=1, keepdims=True)
    total = jnp.sum(scores * hot[...], axis=0, keepdims=True)
    out[...] = jnp.broadcast_to(total, out.shape)


def final_kernel(parts, prior, out, wide):
    domains = prior.shape[-1]
    share = out.shape[-1]
    total = jnp.sum(parts[...], axis=0, keepdims=True)
    spread = jnp.sqrt(jnp.mean(total * total, axis=1, keepdims=True) + 1e-06)
    half = 0.5 * (total / spread)
    mass = jnp.sum(prior[...] * jnp.exp(half), axis=1, keepdims=True)
    lanes = wide.shape[-1]
    wide[...] = jnp.zeros_like(wide)
    wide[:, :domains] = jnp.log(prior[...]) + half - jnp.log(mass)
    first = lax.axis_index("dp") * share
    out[...] = pltpu.roll(wide[...], lax.rem(lanes - first, lanes), 1)[:, :share]


def per_device(
    dense_act,
    dense_cot,
    dense_proj_in,
    dense_proj_out,
    expert_act,
    expert_cot,
    expert_proj_in,
    expert_proj_out,
    dense_valid,
    expert_valid,
    domain_ids,
    prior_mix,
):
    layers, micro, rows, dwidth = dense_cot.shape
    experts, slots = expert_cot.shape[1:3]
    d_in = dense_act.shape[3]
    e_in = expert_act.shape[3]
    rank = dense_proj_in.shape[2]
    domains = prior_mix.shape[0]
    world = lax.axis_size(AXES)
    n_tensor = lax.axis_size("tensor")
    swap = [(i, i ^ 1) for i in range(n_tensor)]
    f32, bf16 = jnp.float32, jnp.bfloat16
    dma = pltpu.SemaphoreType.DMA

    hbm = functools.partial(pltpu.with_memory_space_constraint, memory_space=pltpu.HBM)
    dense_act, dense_cot, dense_proj_in, dense_proj_out = map(
        hbm, (dense_act, dense_cot, dense_proj_in, dense_proj_out)
    )
    expert_act, expert_cot, expert_proj_in, expert_proj_out = map(
        hbm, (expert_act, expert_cot, expert_proj_in, expert_proj_out)
    )
    dense_valid, expert_valid = hbm(dense_valid), hbm(expert_valid)

    e_send = pl.pallas_call(
        expert_send_kernel,
        out_shape=jax.ShapeDtypeStruct((micro, experts, slots, rank), f32),
        in_specs=[HBM, HBM],
        out_specs=VMEM,
        scratch_shapes=[
            pltpu.VMEM((micro, experts, slots, e_in), bf16),
            pltpu.VMEM((e_in, rank), bf16),
            dma((micro + 1,)),
        ],
        compiler_params=vmem(4),
        name="expert_send",
    )(expert_act, expert_proj_in)
    e_got = lax.ppermute(e_send, "tensor", swap)

    d_send = pl.pallas_call(
        dense_send_kernel,
        out_shape=jax.ShapeDtypeStruct((layers, micro, rows, rank), f32),
        in_specs=[HBM, HBM, ANY],
        out_specs=VMEM,
        scratch_shapes=[
            pltpu.VMEM((layers, micro, rows, d_in), bf16),
            pltpu.VMEM((layers, d_in, rank), bf16),
            dma((layers * (micro + 1),)),
        ],
        compiler_params=vmem(8),
        name="dense_send",
    )(dense_act, dense_proj_in, e_send)
    d_got = lax.ppermute(d_send, "tensor", swap)

    y_d, y_e, own, hot = pl.pallas_call(
        own_kernel,
        out_shape=[
            jax.ShapeDtypeStruct((layers, micro, rows, rank), f32),
            jax.ShapeDtypeStruct((micro, experts, slots, rank), f32),
            jax.ShapeDtypeStruct((micro, rank), f32),
            jax.ShapeDtypeStruct((micro, domains), f32),
        ],
        in_specs=[SMEM] + [HBM] * 10,
        out_specs=[VMEM] * 4,
        scratch_shapes=[
            pltpu.VMEM((layers, micro, rows, d_in), bf16),
            pltpu.VMEM((layers, micro, rows, dwidth), bf16),
            pltpu.VMEM((layers, d_in, rank), bf16),
            pltpu.VMEM((layers, dwidth, rank), bf16),
            pltpu.VMEM((micro, experts, slots, e_in), bf16),
            pltpu.VMEM((micro, experts, slots, dwidth), bf16),
            pltpu.VMEM((e_in, rank), bf16),
            pltpu.VMEM((dwidth, rank), bf16),
            pltpu.VMEM((layers, rank, rank), f32),
            pltpu.VMEM((experts, rank, rank), f32),
            dma((layers * (3 + 2 * micro) + 3 + 2 * micro,)),
        ],
        compiler_params=vmem(32),
        name="own_part",
    )(
        domain_ids, dense_act, dense_cot, dense_proj_in, dense_proj_out,
        expert_act, expert_cot, expert_proj_in, expert_proj_out, dense_valid, expert_valid,
    )

    parts = pl.pallas_call(
        combine_kernel,
        out_shape=jax.ShapeDtypeStruct((world, domains), f32),
        in_specs=[VMEM] * 6,
        out_specs=VMEM,
        compiler_params=vmem(6),
        name="combine",
    )(own, hot, d_got, y_d, e_got, y_e)
    parts = lax.all_to_all(parts, AXES, 0, 0, tiled=True)

    share = domains // lax.axis_size("dp")
    lanes = -(-domains // 128) * 128
    out = pl.pallas_call(
        final_kernel,
        out_shape=jax.ShapeDtypeStruct((1, share), f32),
        in_specs=[VMEM, VMEM],
        out_specs=VMEM,
        scratch_shapes=[pltpu.VMEM((1, lanes), f32)],
        compiler_params=vmem(1),
        name="final",
    )(parts, prior_mix.reshape(1, domains))
    return out.reshape(share)


def solution(mesh):
    placed = (
        P(None, "dp", "expert", "tensor"),
        P(None, "dp", ("expert", "tensor"), None),
        P(None, "tensor", None),
        P(),
        P("dp", "expert", None, "tensor"),
        P("dp", "expert", "tensor", None),
        P("tensor", None),
        P(),
        P(),
        P("expert", None, None),
        P("dp"),
        P(),
    )

    return jax.shard_map(per_device, mesh=mesh, in_specs=placed, out_specs=P("dp"), check_vma=False)
```

```python
import functools

import jax
import jax.numpy as jnp
from jax import lax
from jax.experimental import pallas as pl
from jax.experimental.pallas import tpu as pltpu
from jax.sharding import PartitionSpec as P


AXES = ("dp", "expert", "tensor")
GROUP = 2
HBM = pl.BlockSpec(memory_space=pltpu.HBM)
ANY = pl.BlockSpec(memory_space=pl.ANY)
VMEM = pl.BlockSpec(memory_space=pltpu.VMEM)
SMEM = pl.BlockSpec(memory_space=pltpu.SMEM)


def vmem(mib):
    return pltpu.CompilerParams(vmem_limit_bytes=mib * 2**20)


def start_all(pairs, sems):
    copies = [pltpu.make_async_copy(src, dst, sems.at[i]) for i, (src, dst) in enumerate(pairs)]
    for copy in copies:
        copy.start()
    return copies


def dot(a, b):
    return jnp.dot(a, b, preferred_element_type=jnp.float32)


def dot_exact(a, b):
    return lax.dot_general(
        a, b, (((1,), (1,)), ((), ())), precision=lax.Precision.HIGHEST, preferred_element_type=jnp.float32
    )


def send_kernel(pieces, e_act, e_proj, d_act, d_proj, *rest):
    n = len(pieces)
    sems = rest[-1]
    acts, projs = rest[-1 - 2 * n : -1 - n], rest[-1 - n : -1]
    out = rest[-2 - 2 * n]
    other = 1 - lax.axis_index("tensor")
    pairs = []
    for (layer, first, many), act_v, proj_v in zip(pieces, acts, projs):
        rows = act_v.shape[-2]
        here = pl.ds(other * rows, rows)
        if layer is None:
            pairs += [(e_proj, proj_v), (e_act.at[pl.ds(first, many), :, here, :], act_v)]
        else:
            pairs += [(d_proj.at[layer], proj_v), (d_act.at[layer, pl.ds(first, many), here, :], act_v)]
    copies = iter(start_all(pairs, sems))
    start = 0
    for act_v, proj_v in zip(acts, projs):
        next(copies).wait()
        next(copies).wait()
        u = dot(act_v[...].reshape(-1, act_v.shape[-1]), proj_v[...])
        out[start : start + u.shape[0], :] = u
        start += u.shape[0]


def own_kernel(
    ids, dact, dcot, dpin, dpout, eact, ecot, epin, epout, dval, evaldn,
    yd, ye, own, hot,
    dact_v, dcot_v, dpin_v, dpout_v, eact_v, ecot_v, epin_v, epout_v, dval_v, eval_v, sems,
):
    layers, micro, rows, dwidth = dact_v.shape
    _, experts, slots, ewidth = eact_v.shape
    rank = dval_v.shape[-1]
    tensor = lax.axis_index("tensor")
    groups = [pl.ds(g, GROUP) for g in range(0, micro, GROUP)]
    pairs = [(epout, epout_v), (evaldn, eval_v), (epin, epin_v)]
    for g in groups:
        pairs += [
            (ecot.at[g], ecot_v.at[g]),
            (eact.at[g, :, pl.ds(tensor * slots, slots), :], eact_v.at[g]),
        ]
    for l in range(layers):
        pairs += [(dpout.at[l], dpout_v.at[l]), (dval.at[l], dval_v.at[l]), (dpin.at[l], dpin_v.at[l])]
        for g in groups:
            pairs += [
                (dcot.at[l, g], dcot_v.at[l, g]),
                (dact.at[l, g, pl.ds(tensor * rows, rows), :], dact_v.at[l, g]),
            ]
    copies = iter(start_all(pairs, sems))
    totals = [jnp.zeros((1, rank), jnp.float32) for _ in range(micro)]
    for _ in range(3):
        next(copies).wait()
    for first in range(0, micro, GROUP):
        next(copies).wait()
        w = dot(ecot_v[first : first + GROUP].reshape(GROUP * experts * slots, -1), epout_v[...])
        next(copies).wait()
        u = dot(eact_v[first : first + GROUP].reshape(GROUP * experts * slots, ewidth), epin_v[...])
        for e in range(experts):
            places = [slice((m * experts + e) * slots, (m * experts + e + 1) * slots) for m in range(GROUP)]
            y = dot_exact(jnp.concatenate([w[place] for place in places], axis=0), eval_v[e])
            for m in range(GROUP):
                y_m = y[m * slots : (m + 1) * slots]
                ye[first + m, e] = y_m
                totals[first + m] = totals[first + m] + jnp.sum(u[places[m]] * y_m, axis=0, keepdims=True)
    for l in range(layers):
        for _ in range(3):
            next(copies).wait()
        for first in range(0, micro, GROUP):
            next(copies).wait()
            w = dot(dcot_v[l, first : first + GROUP].reshape(GROUP * rows, -1), dpout_v[l])
            next(copies).wait()
            u = dot(dact_v[l, first : first + GROUP].reshape(GROUP * rows, dwidth), dpin_v[l])
            y = dot_exact(w, dval_v[l])
            for m in range(GROUP):
                place = slice(m * rows, (m + 1) * rows)
                yd[l, first + m] = y[place]
                totals[first + m] = totals[first + m] + jnp.sum(u[place] * y[place], axis=0, keepdims=True)
    own[...] = jnp.concatenate(totals, axis=0)
    lane = lax.broadcasted_iota(jnp.int32, (1, hot.shape[1]), 1)
    for m in range(micro):
        hot[pl.ds(m, 1), :] = (lane == ids[m]).astype(jnp.float32)


def combine_kernel(chunks, own, hot, yd, ye, *rest):
    *got, out = rest
    micro, _ = yd.shape[1:3]
    experts, slots, rank = ye.shape[1:]
    parts = [own[pl.ds(m, 1), :] for m in range(micro)]
    for pieces, u in zip(chunks, got):
        start = 0
        for layer, first, many in pieces:
            for m in range(first, first + many):
                y = ye[m].reshape(experts * slots, rank) if layer is None else yd[layer, m]
                part = u[start : start + y.shape[0], :] * y
                parts[m] = parts[m] + jnp.sum(part, axis=0, keepdims=True)
                start += y.shape[0]
    scores = jnp.sum(jnp.concatenate(parts, axis=0), axis=1, keepdims=True)
    total = jnp.sum(scores * hot[...], axis=0, keepdims=True)
    out[...] = jnp.broadcast_to(total, out.shape)


def final_kernel(parts, prior, out, wide):
    domains = prior.shape[-1]
    share = out.shape[-1]
    total = jnp.sum(parts[...], axis=0, keepdims=True)
    spread = jnp.sqrt(jnp.mean(total * total, axis=1, keepdims=True) + 1e-06)
    half = 0.5 * (total / spread)
    mass = jnp.sum(prior[...] * jnp.exp(half), axis=1, keepdims=True)
    lanes = wide.shape[-1]
    wide[...] = jnp.zeros_like(wide)
    wide[:, :domains] = jnp.log(prior[...]) + half
    first = lax.axis_index("dp") * share
    rolled = pltpu.roll(wide[...], lax.rem(lanes - first, lanes), 1)
    out[...] = rolled[:, :share] - jnp.log(mass)


def per_device(
    dense_act,
    dense_cot,
    dense_proj_in,
    dense_proj_out,
    expert_act,
    expert_cot,
    expert_proj_in,
    expert_proj_out,
    dense_valid,
    expert_valid,
    domain_ids,
    prior_mix,
):
    layers, micro, rows, dwidth = dense_cot.shape
    experts, slots = expert_cot.shape[1:3]
    d_in = dense_act.shape[3]
    e_in = expert_act.shape[3]
    rank = dense_proj_in.shape[2]
    domains = prior_mix.shape[0]
    world = lax.axis_size(AXES)
    n_tensor = lax.axis_size("tensor")
    swap = [(i, i ^ 1) for i in range(n_tensor)]
    f32, bf16 = jnp.float32, jnp.bfloat16
    dma = pltpu.SemaphoreType.DMA

    hbm = functools.partial(pltpu.with_memory_space_constraint, memory_space=pltpu.HBM)
    dense_act, dense_cot, dense_proj_in, dense_proj_out = map(
        hbm, (dense_act, dense_cot, dense_proj_in, dense_proj_out)
    )
    expert_act, expert_cot, expert_proj_in, expert_proj_out = map(
        hbm, (expert_act, expert_cot, expert_proj_in, expert_proj_out)
    )
    dense_valid, expert_valid = hbm(dense_valid), hbm(expert_valid)

    half = micro // 2
    chunks = [
        [(None, 0, half)],
        [(None, half, micro - half), (0, 0, half)],
        [(0, half, micro - half)] + [(l, 0, micro) for l in range(1, layers)],
    ]
    got = []
    after = []
    for pieces in chunks:
        n_rows = sum(many * (experts * slots if layer is None else rows) for layer, _, many in pieces)
        acts = [
            pltpu.VMEM((many, experts, slots, e_in) if layer is None else (many, rows, d_in), bf16)
            for layer, _, many in pieces
        ]
        projs = [pltpu.VMEM((e_in if layer is None else d_in, rank), bf16) for layer, _, _ in pieces]
        sent = pl.pallas_call(
            functools.partial(send_kernel, pieces),
            out_shape=jax.ShapeDtypeStruct((n_rows, rank), f32),
            in_specs=[HBM] * 4 + [ANY] * len(after),
            out_specs=VMEM,
            scratch_shapes=acts + projs + [dma((2 * len(pieces),))],
            compiler_params=vmem(8),
        )(expert_act, expert_proj_in, dense_act, dense_proj_in, *after)
        got.append(lax.ppermute(sent, "tensor", swap))
        after = [sent]

    y_d, y_e, own, hot = pl.pallas_call(
        own_kernel,
        out_shape=[
            jax.ShapeDtypeStruct((layers, micro, rows, rank), f32),
            jax.ShapeDtypeStruct((micro, experts, slots, rank), f32),
            jax.ShapeDtypeStruct((micro, rank), f32),
            jax.ShapeDtypeStruct((micro, domains), f32),
        ],
        in_specs=[SMEM] + [HBM] * 10,
        out_specs=[VMEM] * 4,
        scratch_shapes=[
            pltpu.VMEM((layers, micro, rows, d_in), bf16),
            pltpu.VMEM((layers, micro, rows, dwidth), bf16),
            pltpu.VMEM((layers, d_in, rank), bf16),
            pltpu.VMEM((layers, dwidth, rank), bf16),
            pltpu.VMEM((micro, experts, slots, e_in), bf16),
            pltpu.VMEM((micro, experts, slots, dwidth), bf16),
            pltpu.VMEM((e_in, rank), bf16),
            pltpu.VMEM((dwidth, rank), bf16),
            pltpu.VMEM((layers, rank, rank), f32),
            pltpu.VMEM((experts, rank, rank), f32),
            dma(((layers + 1) * (3 + 2 * (micro // GROUP)),)),
        ],
        compiler_params=vmem(32),
        name="own_part",
    )(
        domain_ids, dense_act, dense_cot, dense_proj_in, dense_proj_out,
        expert_act, expert_cot, expert_proj_in, expert_proj_out, dense_valid, expert_valid,
    )

    parts = pl.pallas_call(
        functools.partial(combine_kernel, chunks),
        out_shape=jax.ShapeDtypeStruct((world, domains), f32),
        in_specs=[VMEM] * (4 + len(got)),
        out_specs=VMEM,
        compiler_params=vmem(6),
        name="combine",
    )(own, hot, y_d, y_e, *got)
    parts = lax.all_to_all(parts, AXES, 0, 0, tiled=True)

    share = domains // lax.axis_size("dp")
    lanes = -(-domains // 128) * 128
    out = pl.pallas_call(
        final_kernel,
        out_shape=jax.ShapeDtypeStruct((1, share), f32),
        in_specs=[VMEM, VMEM],
        out_specs=VMEM,
        scratch_shapes=[pltpu.VMEM((1, lanes), f32)],
        compiler_params=vmem(1),
        name="final",
    )(parts, prior_mix.reshape(1, domains))
    return out.reshape(share)


def solution(mesh):
    placed = (
        P(None, "dp", "expert", "tensor"),
        P(None, "dp", ("expert", "tensor"), None),
        P(None, "tensor", None),
        P(),
        P("dp", "expert", None, "tensor"),
        P("dp", "expert", "tensor", None),
        P("tensor", None),
        P(),
        P(),
        P("expert", None, None),
        P("dp"),
        P(),
    )

    return jax.shard_map(per_device, mesh=mesh, in_specs=placed, out_specs=P("dp"), check_vma=False)
```

```python
import functools

import jax
import jax.numpy as jnp
from jax import lax
from jax.experimental import pallas as pl
from jax.experimental.pallas import tpu as pltpu
from jax.sharding import PartitionSpec as P


AXES = ("dp", "expert", "tensor")
GROUP = 2
HBM = pl.BlockSpec(memory_space=pltpu.HBM)
ANY = pl.BlockSpec(memory_space=pl.ANY)
VMEM = pl.BlockSpec(memory_space=pltpu.VMEM)
SMEM = pl.BlockSpec(memory_space=pltpu.SMEM)


def vmem(mib):
    return pltpu.CompilerParams(vmem_limit_bytes=mib * 2**20)


def start_all(pairs, sems):
    copies = [pltpu.make_async_copy(src, dst, sems.at[i]) for i, (src, dst) in enumerate(pairs)]
    for copy in copies:
        copy.start()
    return copies


def dot(a, b):
    return jnp.dot(a, b, preferred_element_type=jnp.float32)


def dot_exact(a, b):
    return lax.dot_general(
        a, b, (((1,), (1,)), ((), ())), precision=lax.Precision.HIGHEST, preferred_element_type=jnp.float32
    )


def send_kernel(pieces, e_act, e_proj, d_act, d_proj, *rest):
    n = len(pieces)
    sems = rest[-1]
    acts, projs = rest[-1 - 2 * n : -1 - n], rest[-1 - n : -1]
    out = rest[-2 - 2 * n]
    other = 1 - lax.axis_index("tensor")
    pairs = []
    for (layer, first, many), act_v, proj_v in zip(pieces, acts, projs):
        rows = act_v.shape[-2]
        here = pl.ds(other * rows, rows)
        if layer is None:
            pairs += [(e_proj, proj_v), (e_act.at[pl.ds(first, many), :, here, :], act_v)]
        else:
            pairs += [(d_proj.at[layer], proj_v), (d_act.at[layer, pl.ds(first, many), here, :], act_v)]
    copies = iter(start_all(pairs, sems))
    start = 0
    for act_v, proj_v in zip(acts, projs):
        next(copies).wait()
        next(copies).wait()
        u = dot(act_v[...].reshape(-1, act_v.shape[-1]), proj_v[...])
        out[start : start + u.shape[0], :] = u
        start += u.shape[0]


def is_second():
    return lax.axis_index("expert") == lax.axis_size("expert") - 1


def expert_kernel(second, eact, ecot, epin, epout, evaldn, *rest):
    ye, own, eact_v, epin_v, eval_v, sems = rest[-6:]
    micro, experts, slots, ewidth = eact_v.shape
    rank = eval_v.shape[-1]

    def work():
        here = pl.ds(lax.axis_index("tensor") * slots, slots)
        groups = [pl.ds(g, GROUP) for g in range(0, micro, GROUP)]
        pairs = [(epin, epin_v), (evaldn, eval_v)]
        pairs += [(eact.at[g, :, here, :], eact_v.at[g]) for g in groups]
        copies = iter(start_all(pairs, sems))
        ws = [
            dot(ecot[first : first + GROUP].reshape(GROUP * experts * slots, -1), epout[...])
            for first in range(0, micro, GROUP)
        ]
        next(copies).wait()
        next(copies).wait()
        for first, w in zip(range(0, micro, GROUP), ws):
            next(copies).wait()
            u = dot(eact_v[first : first + GROUP].reshape(GROUP * experts * slots, ewidth), epin_v[...])
            totals = [jnp.zeros((1, rank), jnp.float32) for _ in range(GROUP)]
            for e in range(experts):
                places = [slice((m * experts + e) * slots, (m * experts + e + 1) * slots) for m in range(GROUP)]
                y = dot_exact(jnp.concatenate([w[place] for place in places], axis=0), eval_v[e])
                for m in range(GROUP):
                    y_m = y[m * slots : (m + 1) * slots]
                    ye[first + m, e] = y_m
                    totals[m] = totals[m] + jnp.sum(u[places[m]] * y_m, axis=0, keepdims=True)
            for m in range(GROUP):
                own[pl.ds(first + m, 1), :] = totals[m]

    def idle():
        ye[...] = jnp.zeros_like(ye)
        own[...] = jnp.zeros_like(own)

    lax.cond(is_second() if second else jnp.logical_not(is_second()), work, idle)


def own_kernel(
    ids, dact, dcot, dpin, dpout, dval,
    yd, own, hot,
    dact_v, dpin_v, dval_v, sems,
):
    layers, micro, rows, dwidth = dact_v.shape
    rank = dval_v.shape[-1]
    here = pl.ds(lax.axis_index("tensor") * rows, rows)
    groups = [pl.ds(g, GROUP) for g in range(0, micro, GROUP)]
    pairs = []
    for l in range(layers):
        pairs += [(dval.at[l], dval_v.at[l]), (dpin.at[l], dpin_v.at[l])]
        pairs += [(dact.at[l, g, here, :], dact_v.at[l, g]) for g in groups]
    copies = iter(start_all(pairs, sems))
    totals = [jnp.zeros((1, rank), jnp.float32) for _ in range(micro)]
    for l in range(layers):
        w_l = [
            dot(dcot[l, first : first + GROUP].reshape(GROUP * rows, -1), dpout[l])
            for first in range(0, micro, GROUP)
        ]
        next(copies).wait()
        next(copies).wait()
        for first, w in zip(range(0, micro, GROUP), w_l):
            next(copies).wait()
            u = dot(dact_v[l, first : first + GROUP].reshape(GROUP * rows, dwidth), dpin_v[l])
            y = dot_exact(w, dval_v[l])
            for m in range(GROUP):
                place = slice(m * rows, (m + 1) * rows)
                yd[l, first + m] = y[place]
                totals[first + m] = totals[first + m] + jnp.sum(u[place] * y[place], axis=0, keepdims=True)
    own[...] = jnp.concatenate(totals, axis=0)
    lane = lax.broadcasted_iota(jnp.int32, (1, hot.shape[1]), 1)
    for m in range(micro):
        hot[pl.ds(m, 1), :] = (lane == ids[m]).astype(jnp.float32)


def combine_kernel(chunks, own, hot, yd, ye, own_e, ye_early, own_early, *rest):
    *got, out = rest
    micro, _ = yd.shape[1:3]
    experts, slots, rank = ye.shape[1:]
    parts = [own[pl.ds(m, 1), :] + own_e[pl.ds(m, 1), :] + own_early[pl.ds(m, 1), :] for m in range(micro)]
    for pieces, u in zip(chunks, got):
        start = 0
        for layer, first, many in pieces:
            for m in range(first, first + many):
                y = (ye[m] + ye_early[m]).reshape(experts * slots, rank) if layer is None else yd[layer, m]
                part = u[start : start + y.shape[0], :] * y
                parts[m] = parts[m] + jnp.sum(part, axis=0, keepdims=True)
                start += y.shape[0]
    scores = jnp.sum(jnp.concatenate(parts, axis=0), axis=1, keepdims=True)
    total = jnp.sum(scores * hot[...], axis=0, keepdims=True)
    out[...] = jnp.broadcast_to(total, out.shape)


def final_kernel(parts, prior, out, wide):
    domains = prior.shape[-1]
    share = out.shape[-1]
    total = jnp.sum(parts[...], axis=0, keepdims=True)
    spread = jnp.sqrt(jnp.mean(total * total, axis=1, keepdims=True) + 1e-06)
    half = 0.5 * (total / spread)
    mass = jnp.sum(prior[...] * jnp.exp(half), axis=1, keepdims=True)
    lanes = wide.shape[-1]
    wide[...] = jnp.zeros_like(wide)
    wide[:, :domains] = jnp.log(prior[...]) + half
    first = lax.axis_index("dp") * share
    rolled = pltpu.roll(wide[...], lax.rem(lanes - first, lanes), 1)
    out[...] = rolled[:, :share] - jnp.log(mass)


def per_device(
    dense_act,
    dense_cot,
    dense_proj_in,
    dense_proj_out,
    expert_act,
    expert_cot,
    expert_proj_in,
    expert_proj_out,
    dense_valid,
    expert_valid,
    domain_ids,
    prior_mix,
):
    layers, micro, rows, _ = dense_cot.shape
    experts, slots = expert_cot.shape[1:3]
    d_in = dense_act.shape[3]
    e_in = expert_act.shape[3]
    rank = dense_proj_in.shape[2]
    domains = prior_mix.shape[0]
    world = lax.axis_size(AXES)
    n_tensor = lax.axis_size("tensor")
    swap = [(i, i ^ 1) for i in range(n_tensor)]
    f32, bf16 = jnp.float32, jnp.bfloat16
    dma = pltpu.SemaphoreType.DMA

    hbm = functools.partial(pltpu.with_memory_space_constraint, memory_space=pltpu.HBM)
    near = functools.partial(pltpu.with_memory_space_constraint, memory_space=pltpu.VMEM)
    dense_act, dense_proj_in, expert_act, expert_proj_in = map(
        hbm, (dense_act, dense_proj_in, expert_act, expert_proj_in)
    )
    dense_cot, dense_proj_out, expert_cot, expert_proj_out = map(
        near, (dense_cot, dense_proj_out, expert_cot, expert_proj_out)
    )
    dense_valid, expert_valid = hbm(dense_valid), hbm(expert_valid)

    half = micro // 2
    chunks = [
        [(None, 0, half)],
        [(None, half, micro - half), (0, 0, half)],
        [(0, half, micro - half)] + [(l, 0, micro) for l in range(1, layers)],
    ]
    e_out = [
        jax.ShapeDtypeStruct((micro, experts, slots, rank), f32),
        jax.ShapeDtypeStruct((micro, rank), f32),
    ]

    def expert_part(second, after):
        return pl.pallas_call(
            functools.partial(expert_kernel, second),
            out_shape=e_out,
            in_specs=[HBM, VMEM, HBM, VMEM, HBM] + [ANY] * len(after),
            out_specs=[VMEM] * 2,
            scratch_shapes=[
                pltpu.VMEM((micro, experts, slots, e_in), bf16),
                pltpu.VMEM((e_in, rank), bf16),
                pltpu.VMEM((experts, rank, rank), f32),
                dma((2 + micro // GROUP,)),
            ],
            compiler_params=vmem(12),
        )(expert_act, expert_cot, expert_proj_in, expert_proj_out, expert_valid, *after)

    got = []
    after = []
    for i, pieces in enumerate(chunks):
        n_rows = sum(many * (experts * slots if layer is None else rows) for layer, _, many in pieces)
        acts = [
            pltpu.VMEM((many, experts, slots, e_in) if layer is None else (many, rows, d_in), bf16)
            for layer, _, many in pieces
        ]
        projs = [pltpu.VMEM((e_in if layer is None else d_in, rank), bf16) for layer, _, _ in pieces]
        if i == len(chunks) - 1:
            y_early, own_early = expert_part(True, after)
            after = [own_early]
        sent = pl.pallas_call(
            functools.partial(send_kernel, pieces),
            out_shape=jax.ShapeDtypeStruct((n_rows, rank), f32),
            in_specs=[HBM] * 4 + [ANY] * len(after),
            out_specs=VMEM,
            scratch_shapes=acts + projs + [dma((2 * len(pieces),))],
            compiler_params=vmem(8),
        )(expert_act, expert_proj_in, dense_act, dense_proj_in, *after)
        got.append(lax.ppermute(sent, "tensor", swap))
        after = [sent]

    y_e, own_e = expert_part(False, [sent])
    y_d, own, hot = pl.pallas_call(
        own_kernel,
        out_shape=[
            jax.ShapeDtypeStruct((layers, micro, rows, rank), f32),
            jax.ShapeDtypeStruct((micro, rank), f32),
            jax.ShapeDtypeStruct((micro, domains), f32),
        ],
        in_specs=[SMEM, HBM, VMEM, HBM, VMEM, HBM],
        out_specs=[VMEM] * 3,
        scratch_shapes=[
            pltpu.VMEM((layers, micro, rows, d_in), bf16),
            pltpu.VMEM((layers, d_in, rank), bf16),
            pltpu.VMEM((layers, rank, rank), f32),
            dma((layers * (2 + micro // GROUP),)),
        ],
        compiler_params=vmem(20),
        name="own_part",
    )(domain_ids, dense_act, dense_cot, dense_proj_in, dense_proj_out, dense_valid)

    parts = pl.pallas_call(
        functools.partial(combine_kernel, chunks),
        out_shape=jax.ShapeDtypeStruct((world, domains), f32),
        in_specs=[VMEM] * (7 + len(got)),
        out_specs=VMEM,
        compiler_params=vmem(6),
        name="combine",
    )(own, hot, y_d, y_e, own_e, y_early, own_early, *got)
    parts = lax.all_to_all(parts, AXES, 0, 0, tiled=True)

    share = domains // lax.axis_size("dp")
    lanes = -(-domains // 128) * 128
    out = pl.pallas_call(
        final_kernel,
        out_shape=jax.ShapeDtypeStruct((1, share), f32),
        in_specs=[VMEM, VMEM],
        out_specs=VMEM,
        scratch_shapes=[pltpu.VMEM((1, lanes), f32)],
        compiler_params=vmem(1),
        name="final",
    )(parts, prior_mix.reshape(1, domains))
    return out.reshape(share)


def solution(mesh):
    placed = (
        P(None, "dp", "expert", "tensor"),
        P(None, "dp", ("expert", "tensor"), None),
        P(None, "tensor", None),
        P(),
        P("dp", "expert", None, "tensor"),
        P("dp", "expert", "tensor", None),
        P("tensor", None),
        P(),
        P(),
        P("expert", None, None),
        P("dp"),
        P(),
    )

    return jax.shard_map(per_device, mesh=mesh, in_specs=placed, out_specs=P("dp"), check_vma=False)
```

```python
import functools

import jax
import jax.numpy as jnp
from jax import lax
from jax.experimental import pallas as pl
from jax.experimental.pallas import tpu as pltpu
from jax.sharding import PartitionSpec as P


AXES = ("dp", "expert", "tensor")
GROUP = 2
HBM = pl.BlockSpec(memory_space=pltpu.HBM)
ANY = pl.BlockSpec(memory_space=pl.ANY)
VMEM = pl.BlockSpec(memory_space=pltpu.VMEM)
SMEM = pl.BlockSpec(memory_space=pltpu.SMEM)


def vmem(mib):
    return pltpu.CompilerParams(vmem_limit_bytes=mib * 2**20)


def start_all(pairs, sems):
    copies = [pltpu.make_async_copy(src, dst, sems.at[i]) for i, (src, dst) in enumerate(pairs)]
    for copy in copies:
        copy.start()
    return copies


def dot(a, b):
    return jnp.dot(a, b, preferred_element_type=jnp.float32)


def dot_exact(a, b):
    return lax.dot_general(
        a, b, (((1,), (1,)), ((), ())), precision=lax.Precision.HIGHEST, preferred_element_type=jnp.float32
    )


def send_kernel(pieces, e_act, e_proj, d_act, d_proj, *rest):
    n = len(pieces)
    sems = rest[-1]
    acts, projs = rest[-1 - 2 * n : -1 - n], rest[-1 - n : -1]
    out = rest[-2 - 2 * n]
    other = 1 - lax.axis_index("tensor")
    pairs = []
    for (layer, first, many), act_v, proj_v in zip(pieces, acts, projs):
        rows = act_v.shape[-2]
        here = pl.ds(other * rows, rows)
        if layer is None:
            pairs += [(e_proj, proj_v), (e_act.at[pl.ds(first, many), :, here, :], act_v)]
        else:
            pairs += [(d_proj.at[layer], proj_v), (d_act.at[layer, pl.ds(first, many), here, :], act_v)]
    copies = iter(start_all(pairs, sems))
    start = 0
    for act_v, proj_v in zip(acts, projs):
        next(copies).wait()
        next(copies).wait()
        u = dot(act_v[...].reshape(-1, act_v.shape[-1]), proj_v[...])
        out[start : start + u.shape[0], :] = u
        start += u.shape[0]


def is_second():
    return lax.axis_index("expert") == lax.axis_size("expert") - 1


def expert_kernel(second, eact, ecot, epin, epout, evaldn, *rest):
    ye, own, eact_v, epin_v, eval_v, sems = rest[-6:]
    micro, experts, slots, ewidth = eact_v.shape
    rank = eval_v.shape[-1]

    def work():
        here = pl.ds(lax.axis_index("tensor") * slots, slots)
        groups = [pl.ds(g, GROUP) for g in range(0, micro, GROUP)]
        pairs = [(epin, epin_v), (evaldn, eval_v)]
        pairs += [(eact.at[g, :, here, :], eact_v.at[g]) for g in groups]
        copies = iter(start_all(pairs, sems))
        ws = [
            dot(ecot[first : first + GROUP].reshape(GROUP * experts * slots, -1), epout[...])
            for first in range(0, micro, GROUP)
        ]
        next(copies).wait()
        next(copies).wait()
        for first, w in zip(range(0, micro, GROUP), ws):
            next(copies).wait()
            u = dot(eact_v[first : first + GROUP].reshape(GROUP * experts * slots, ewidth), epin_v[...])
            totals = [jnp.zeros((1, rank), jnp.float32) for _ in range(GROUP)]
            for e in range(experts):
                places = [slice((m * experts + e) * slots, (m * experts + e + 1) * slots) for m in range(GROUP)]
                y = dot_exact(jnp.concatenate([w[place] for place in places], axis=0), eval_v[e])
                for m in range(GROUP):
                    y_m = y[m * slots : (m + 1) * slots]
                    ye[first + m, e] = y_m
                    totals[m] = totals[m] + jnp.sum(u[places[m]] * y_m, axis=0, keepdims=True)
            for m in range(GROUP):
                own[pl.ds(first + m, 1), :] = totals[m]

    def idle():
        ye[...] = jnp.zeros_like(ye)
        own[...] = jnp.zeros_like(own)

    lax.cond(is_second() if second else jnp.logical_not(is_second()), work, idle)


def own_kernel(
    ids, dact, dcot, dpin, dpout, dval,
    yd, own, hot,
    dact_v, dpin_v, dval_v, sems,
):
    layers, micro, rows, dwidth = dact_v.shape
    rank = dval_v.shape[-1]
    here = pl.ds(lax.axis_index("tensor") * rows, rows)
    groups = [pl.ds(g, GROUP) for g in range(0, micro, GROUP)]
    pairs = []
    for l in range(layers):
        pairs += [(dval.at[l], dval_v.at[l]), (dpin.at[l], dpin_v.at[l])]
        pairs += [(dact.at[l, g, here, :], dact_v.at[l, g]) for g in groups]
    copies = iter(start_all(pairs, sems))
    totals = [jnp.zeros((1, rank), jnp.float32) for _ in range(micro)]
    for l in range(layers):
        w_l = [
            dot(dcot[l, first : first + GROUP].reshape(GROUP * rows, -1), dpout[l])
            for first in range(0, micro, GROUP)
        ]
        next(copies).wait()
        next(copies).wait()
        for first, w in zip(range(0, micro, GROUP), w_l):
            next(copies).wait()
            u = dot(dact_v[l, first : first + GROUP].reshape(GROUP * rows, dwidth), dpin_v[l])
            y = dot_exact(w, dval_v[l])
            for m in range(GROUP):
                place = slice(m * rows, (m + 1) * rows)
                yd[l, first + m] = y[place]
                totals[first + m] = totals[first + m] + jnp.sum(u[place] * y[place], axis=0, keepdims=True)
    own[...] = jnp.concatenate(totals, axis=0)
    lane = lax.broadcasted_iota(jnp.int32, (1, hot.shape[1]), 1)
    for m in range(micro):
        hot[pl.ds(m, 1), :] = (lane == ids[m]).astype(jnp.float32)


def received(chunks, got, parts, yd, y_expert):
    for pieces, u in zip(chunks, got):
        start = 0
        for layer, first, many in pieces:
            for m in range(first, first + many):
                y = y_expert(m) if layer is None else yd[layer, m]
                part = u[start : start + y.shape[0], :] * y
                parts[m] = parts[m] + jnp.sum(part, axis=0, keepdims=True)
                start += y.shape[0]
    return parts


def gather_kernel(chunks, own, yd, ye, own_e, ye_early, own_early, *rest):
    *got, out = rest
    micro, experts, slots, rank = ye.shape
    parts = [own[pl.ds(m, 1), :] + own_e[pl.ds(m, 1), :] + own_early[pl.ds(m, 1), :] for m in range(micro)]
    y_expert = lambda m: (ye[m] + ye_early[m]).reshape(experts * slots, rank)
    out[...] = jnp.concatenate(received(chunks, got, parts, yd, y_expert), axis=0)


def combine_kernel(chunk, own, hot, yd, got, out):
    micro = yd.shape[1]
    parts = received([chunk], [got], [own[pl.ds(m, 1), :] for m in range(micro)], yd, None)
    scores = jnp.sum(jnp.concatenate(parts, axis=0), axis=1, keepdims=True)
    total = jnp.sum(scores * hot[...], axis=0, keepdims=True)
    out[...] = jnp.broadcast_to(total, out.shape)


def final_kernel(parts, prior, out, wide):
    domains = prior.shape[-1]
    share = out.shape[-1]
    total = jnp.sum(parts[...], axis=0, keepdims=True)
    per_spread = lax.rsqrt(jnp.mean(total * total, axis=1, keepdims=True) + 1e-06)
    half = total * (0.5 * per_spread)
    mass = jnp.sum(prior[...] * jnp.exp(half), axis=1, keepdims=True)
    lanes = wide.shape[-1]
    wide[:, :domains] = jnp.log(prior[...]) + half
    first = lax.axis_index("dp") * share
    rolled = pltpu.roll(wide[...], lax.rem(lanes - first, lanes), 1)
    out[...] = rolled[:, :share] - jnp.log(mass)


def per_device(
    dense_act,
    dense_cot,
    dense_proj_in,
    dense_proj_out,
    expert_act,
    expert_cot,
    expert_proj_in,
    expert_proj_out,
    dense_valid,
    expert_valid,
    domain_ids,
    prior_mix,
):
    layers, micro, rows, _ = dense_cot.shape
    experts, slots = expert_cot.shape[1:3]
    d_in = dense_act.shape[3]
    e_in = expert_act.shape[3]
    rank = dense_proj_in.shape[2]
    domains = prior_mix.shape[0]
    world = lax.axis_size(AXES)
    n_tensor = lax.axis_size("tensor")
    swap = [(i, i ^ 1) for i in range(n_tensor)]
    f32, bf16 = jnp.float32, jnp.bfloat16
    dma = pltpu.SemaphoreType.DMA

    hbm = functools.partial(pltpu.with_memory_space_constraint, memory_space=pltpu.HBM)
    near = functools.partial(pltpu.with_memory_space_constraint, memory_space=pltpu.VMEM)
    dense_act, dense_proj_in, expert_act, expert_proj_in = map(
        hbm, (dense_act, dense_proj_in, expert_act, expert_proj_in)
    )
    dense_cot, dense_proj_out, expert_cot, expert_proj_out = map(
        near, (dense_cot, dense_proj_out, expert_cot, expert_proj_out)
    )
    dense_valid, expert_valid = hbm(dense_valid), hbm(expert_valid)

    half = micro // 2
    chunks = [
        [(None, 0, half)],
        [(None, half, micro - half), (0, 0, half)],
        [(0, half, micro - half)] + [(l, 0, micro) for l in range(1, layers)],
    ]
    e_out = [
        jax.ShapeDtypeStruct((micro, experts, slots, rank), f32),
        jax.ShapeDtypeStruct((micro, rank), f32),
    ]

    def expert_part(second, after):
        return pl.pallas_call(
            functools.partial(expert_kernel, second),
            out_shape=e_out,
            in_specs=[HBM, VMEM, HBM, VMEM, HBM] + [ANY] * len(after),
            out_specs=[VMEM] * 2,
            scratch_shapes=[
                pltpu.VMEM((micro, experts, slots, e_in), bf16),
                pltpu.VMEM((e_in, rank), bf16),
                pltpu.VMEM((experts, rank, rank), f32),
                dma((2 + micro // GROUP,)),
            ],
            compiler_params=vmem(12),
        )(expert_act, expert_cot, expert_proj_in, expert_proj_out, expert_valid, *after)

    got = []
    after = []
    for i, pieces in enumerate(chunks):
        n_rows = sum(many * (experts * slots if layer is None else rows) for layer, _, many in pieces)
        acts = [
            pltpu.VMEM((many, experts, slots, e_in) if layer is None else (many, rows, d_in), bf16)
            for layer, _, many in pieces
        ]
        projs = [pltpu.VMEM((e_in if layer is None else d_in, rank), bf16) for layer, _, _ in pieces]
        if i == len(chunks) - 1:
            y_early, own_early = expert_part(True, after)
            after = [own_early]
        sent = pl.pallas_call(
            functools.partial(send_kernel, pieces),
            out_shape=jax.ShapeDtypeStruct((n_rows, rank), f32),
            in_specs=[HBM] * 4 + [ANY] * len(after),
            out_specs=VMEM,
            scratch_shapes=acts + projs + [dma((2 * len(pieces),))],
            compiler_params=vmem(8),
        )(expert_act, expert_proj_in, dense_act, dense_proj_in, *after)
        got.append(lax.ppermute(sent, "tensor", swap))
        after = [sent]

    y_e, own_e = expert_part(False, [sent])
    y_d, own, hot = pl.pallas_call(
        own_kernel,
        out_shape=[
            jax.ShapeDtypeStruct((layers, micro, rows, rank), f32),
            jax.ShapeDtypeStruct((micro, rank), f32),
            jax.ShapeDtypeStruct((micro, domains), f32),
        ],
        in_specs=[SMEM, HBM, VMEM, HBM, VMEM, HBM],
        out_specs=[VMEM] * 3,
        scratch_shapes=[
            pltpu.VMEM((layers, micro, rows, d_in), bf16),
            pltpu.VMEM((layers, d_in, rank), bf16),
            pltpu.VMEM((layers, rank, rank), f32),
            dma((layers * (2 + micro // GROUP),)),
        ],
        compiler_params=vmem(20),
        name="own_part",
    )(domain_ids, dense_act, dense_cot, dense_proj_in, dense_proj_out, dense_valid)

    own = pl.pallas_call(
        functools.partial(gather_kernel, chunks[:-1]),
        out_shape=jax.ShapeDtypeStruct((micro, rank), f32),
        in_specs=[VMEM] * (6 + len(got) - 1),
        out_specs=VMEM,
        compiler_params=vmem(6),
        name="gather",
    )(own, y_d, y_e, own_e, y_early, own_early, *got[:-1])
    parts = pl.pallas_call(
        functools.partial(combine_kernel, chunks[-1]),
        out_shape=jax.ShapeDtypeStruct((world, domains), f32),
        in_specs=[VMEM] * 4,
        out_specs=VMEM,
        compiler_params=vmem(6),
        name="combine",
    )(own, hot, y_d, got[-1])
    parts = lax.all_to_all(parts, AXES, 0, 0, tiled=True)

    share = domains // lax.axis_size("dp")
    lanes = -(-domains // 128) * 128
    out = pl.pallas_call(
        final_kernel,
        out_shape=jax.ShapeDtypeStruct((1, share), f32),
        in_specs=[VMEM, VMEM],
        out_specs=VMEM,
        scratch_shapes=[pltpu.VMEM((1, lanes), f32)],
        compiler_params=vmem(1),
        name="final",
    )(parts, prior_mix.reshape(1, domains))
    return out.reshape(share)


def solution(mesh):
    placed = (
        P(None, "dp", "expert", "tensor"),
        P(None, "dp", ("expert", "tensor"), None),
        P(None, "tensor", None),
        P(),
        P("dp", "expert", None, "tensor"),
        P("dp", "expert", "tensor", None),
        P("tensor", None),
        P(),
        P(),
        P("expert", None, None),
        P("dp"),
        P(),
    )

    return jax.shard_map(per_device, mesh=mesh, in_specs=placed, out_specs=P("dp"), check_vma=False)
```
